32 devices in a mesh: gx: 4 (over x, core), gy: 4 (over z), gz: 2 (over y).
Axes of the slice: x: 2, y: 2, z: 4, core: 2. Of those that a mesh axis runs over, the one named last changes fastest.
Arguments:
- in_first: bfloat16 [16384, 1024], P(('gx', 'gy', 'gz')), may hold values from -98 to 98
- cot_first: bfloat16 [16384, 256], P(('gx', 'gy', 'gz')), may hold values from -0.234375 to 0.234375
- in_third: bfloat16 [16384, 256], P(('gx', 'gy', 'gz')), may hold values from -98 to 98
- cot_third: bfloat16 [16384, 1024], P(('gx', 'gy', 'gz')), may hold values from -0.234375 to 0.234375
- mean_old: float32 [524288], P(('gx', 'gy', 'gz')), may hold values from -6 to 6
- prec_old: float32 [524288], P(('gx', 'gy', 'gz')), may hold values from 0.5 to 4
- mom_old: float32 [524288], P(('gx', 'gy', 'gz')), may hold values from -4 to 4
- noise: bfloat16 [32, 524288], P(('gx', 'gy', 'gz')), may hold values from -6 to 6
Outputs:
- mean_new: float32 [524288], P(('gx', 'gy', 'gz'))
- prec_new: float32 [524288], P(('gx', 'gy', 'gz'))
- mom_new: float32 [524288], P(('gx', 'gy', 'gz'))
- samples: bfloat16 [32, 524288], P(('gx', 'gy', 'gz'))
The draws below stay inside these ranges and needn't reach their ends.
All inputs are finite; a program needn't handle non-finite values.
Results may differ from the reference program's by a relative error of at most 0.0016.
Values sent between devices are 32-bit elements; how exact they have to be, the bound alone decides.
A program may use at most 64 MiB of HBM per device.

```python
import math
import jax
import jax.numpy as jnp
from jax import lax

CIN = 1024
MID = 256
TOKENS = 16384
PARAMS = 524288
DEVICES = 32


def section_fields(base_key, row_count, input_cols, output_cols):
    subkeys = jax.random.split(base_key, 7)
    heavy_share = 1.0 / 128.0
    heavy_scale = 5.0
    row_log = jax.random.uniform(subkeys[0], (row_count, 1), jnp.float32, -0.5, 0.5)
    row_tilt = jax.random.uniform(subkeys[1], (row_count, 1), jnp.float32, -1.0, 1.0)
    heavy_pick = jax.random.uniform(subkeys[2], (row_count, 1), jnp.float32, 0.0, 1.0)
    heavy_rows = jnp.where(heavy_pick < heavy_share, heavy_scale, 1.0).astype(jnp.float32)
    input_bend = jax.random.uniform(subkeys[3], (1, input_cols), jnp.float32, -0.5, 0.5)
    output_bend = jax.random.uniform(subkeys[4], (1, output_cols), jnp.float32, -0.5, 0.5)
    input_noise = jnp.clip(jax.random.normal(subkeys[5], (row_count, input_cols), jnp.float32), -6.0, 6.0)
    output_noise = jnp.clip(jax.random.normal(subkeys[6], (row_count, output_cols), jnp.float32), -6.0, 6.0)
    inputs_part = input_noise * heavy_rows * jnp.exp(row_log + row_tilt * input_bend)
    scaling = 0.3 / jnp.sqrt(jnp.float32(row_count))
    cotangents = output_noise * heavy_rows * jnp.exp(row_log + row_tilt * output_bend) * scaling
    return (inputs_part, cotangents)


def draw_in_first(key, part):
    fields = section_fields(jax.random.fold_in(key, 101), TOKENS, CIN, MID)
    return fields[0].astype(jnp.bfloat16)


def draw_cot_first(key, part):
    fields = section_fields(jax.random.fold_in(key, 101), TOKENS, CIN, MID)
    return fields[1].astype(jnp.bfloat16)


def draw_in_third(key, part):
    fields = section_fields(jax.random.fold_in(key, 202), TOKENS, MID, CIN)
    return fields[0].astype(jnp.bfloat16)


def draw_cot_third(key, part):
    fields = section_fields(jax.random.fold_in(key, 202), TOKENS, MID, CIN)
    return fields[1].astype(jnp.bfloat16)


def shard_levels(own_key, dims, cuts, least, largest):
    gain = 1.0
    for dim, shards_of in cuts:
        steps = jax.random.uniform(jax.random.fold_in(jax.random.fold_in(own_key, 6), dim), (shards_of,), jnp.float32, least / len(cuts), largest / len(cuts))
        gain = gain * jnp.repeat(jnp.exp(steps), dims[dim] // shards_of).reshape((-1,) + (1,) * (len(dims) - 1 - dim))
    return gain


def gaussian(own_key, extent, width, bound, cuts=(), held_as=jnp.bfloat16):
    values = jax.random.normal(own_key, extent, jnp.float32) * width
    if len(cuts) > 0:
        values = shard_levels(own_key, extent, cuts, -0.22, 0.18) * values
    return jnp.clip(values, min=-bound, max=bound).astype(held_as)


def setup_inputs(seed: int = 0) -> dict:
    seeds = jax.random.split(jax.random.key(seed), 9)
    return {
        "in_first": draw_in_first(jax.random.fold_in(seeds[8], 71), 0),
        "cot_first": draw_cot_first(jax.random.fold_in(seeds[8], 71), 0),
        "in_third": draw_in_third(jax.random.fold_in(seeds[8], 71), 0),
        "cot_third": draw_cot_third(jax.random.fold_in(seeds[8], 71), 0),
        "mean_old": gaussian(seeds[4], (PARAMS,), 1.0, 6.0, ((0, 32),), jnp.float32),
        "prec_old": jnp.clip(jnp.exp(math.log(4.0) - 2.0794415 * jax.random.uniform(seeds[5], (PARAMS,), jnp.float32) ** shard_levels(seeds[5], (PARAMS,), ((0, 32),), -0.2, 0.2)), 0.5, 4.0),
        "mom_old": gaussian(seeds[6], (PARAMS,), 0.5, 4.0, ((0, 32),), jnp.float32),
        "noise": gaussian(seeds[7], (DEVICES, PARAMS), 1.0, 6.0, ((0, 32),)),
    }


def squared(values):
    wide = values.astype(jnp.float32)
    return (wide * wide).astype(jnp.bfloat16)

def contract_rows(left, right):
    return lax.dot_general(left, right, (((0,), (0,)), ((), ())), preferred_element_type=jnp.float32)

def reference(in_first, cot_first, in_third, cot_third, mean_old, prec_old, mom_old, noise):
    grad_first = contract_rows(in_first, cot_first)
    grad_third = contract_rows(in_third, cot_third)
    curv_first = contract_rows(squared(in_first), squared(cot_first))
    curv_third = contract_rows(squared(in_third), squared(cot_third))
    grad = jnp.concatenate([grad_first.reshape(-1), grad_third.reshape(-1)])
    curv = jnp.concatenate([curv_first.reshape(-1), curv_third.reshape(-1)])
    prec_new = 0.5 * prec_old + 0.5 * curv
    mom_new = 0.9 * mom_old + grad + 0.1 * mean_old
    divisor = prec_new + 0.1 + 0.05
    mean_new = mean_old - 0.3 * mom_new / divisor
    spread = jnp.sqrt(0.3 / divisor)

    def one_sample(noise_row):
        return (mean_new + spread * noise_row.astype(jnp.float32)).astype(jnp.bfloat16)
    samples = lax.map(one_sample, noise)
    return (mean_new, prec_new, mom_new, samples)
```

```python
import functools

import jax
import jax.numpy as jnp
from jax import lax
from jax.experimental import pallas as pl
from jax.experimental.pallas import tpu as pltpu
from jax.sharding import PartitionSpec as P

LANES = 128
BLOCK = 256
AXES = ("gx", "gy", "gz")


def squared(values):
    wide = values.astype(jnp.float32)
    return (wide * wide).astype(jnp.bfloat16)


def contract_rows(left, right):
    return lax.dot_general(
        left, right, (((0,), (0,)), ((), ())), preferred_element_type=jnp.float32
    )


def step_kernel(
    sizes,
    in_first, cot_first, in_third, cot_third, mean_old, prec_old, mom_old,
    mean_out, prec_out, mom_out, gathered,
    part, got_c, sum_f, got_f, sum_g, got_g, sum_z, got_z, divisor,
    c_sems, f_sems, g_sems, z_sems, zz_sems, gg_sems, ff_sems, cc_sems,
):
    X, C, Z, Y, S, splits = sizes
    s = S // splits
    gx, mz, my = (lax.axis_index(name) for name in AXES)
    mx, mc = gx // C, lax.rem(gx, C)
    other_c = 1 - mc

    def device(x=None, c=None, z=None, y=None):
        x = mx if x is None else x
        c = mc if c is None else c
        return (x * C + c, mz if z is None else z, my if y is None else y)

    def away(mine, step, size):
        return lax.rem(mine + step, size)

    barrier = pltpu.get_barrier_semaphore()
    peers = [device(c=other_c)]
    peers += [device(x=away(mx, k, X)) for k in range(1, X)]
    peers += [device(y=away(my, k, Y)) for k in range(1, Y)]
    peers += [device(z=away(mz, k, Z)) for k in range(1, Z)]
    for peer in peers:
        pl.semaphore_signal(barrier, inc=1, device_id=peer, device_id_type=pl.DeviceIdType.MESH)

    started = []

    def link(src, dst, sems, index, peer):
        return pltpu.make_async_remote_copy(
            src_ref=src, dst_ref=dst,
            send_sem=sems.at[(0,) + index], recv_sem=sems.at[(1,) + index],
            device_id=peer, device_id_type=pl.DeviceIdType.MESH,
        )

    def send(*args):
        copy = link(*args)
        copy.start()
        started.append(copy)

    def place(index):
        rest, y = divmod(index, Y)
        rest, z = divmod(rest, Z)
        x, c = divmod(rest, C)
        return x, c, z, y

    def put(kind, base, block, row0, col0, width):
        rows = S * LANES // width
        across = width // LANES
        for i in range(block.shape[0] // rows):
            x, c, z, y = place(base + row0 // rows + i)
            for j in range(block.shape[1] // LANES):
                part[kind, x, c, z, y, pl.ds(col0 // LANES + j, rows, stride=across), :] = (
                    block[i * rows:(i + 1) * rows, j * LANES:(j + 1) * LANES]
                )

    def products(kind, shape):
        cin, mid = in_first.shape[1], cot_first.shape[1]
        right = shape(cot_first[...])
        for r in range(0, cin, BLOCK):
            put(kind, 0, contract_rows(shape(in_first[:, r:r + BLOCK]), right), r, 0, mid)
        base = X * C * Z * Y // 2
        left = shape(in_third[...])
        for r in range(0, cin, BLOCK):
            put(kind, base, contract_rows(left, shape(cot_third[:, r:r + BLOCK])), 0, r, cin)

    pieces = [(kind, split) for kind in (0, 1) for split in range(splits)]
    flip = [(kind + split) % 2 if splits == 1 else split % 2 for kind, split in pieces]

    def rows_of(p):
        split = pieces[p][1]
        return pl.ds(split * s, s)

    def outer(p):
        return (Y, my, X, mx) if flip[p] else (X, mx, Y, my)

    def xy(p, f, g):
        return (g, f) if flip[p] else (f, g)

    def f_peer(p, f):
        return device(y=f) if flip[p] else device(x=f)

    def g_peer(p, g):
        return device(x=g) if flip[p] else device(y=g)

    def c_link(p, i):
        x = away(mx, i + 1, X)
        return (part.at[pieces[p][0], x, other_c, :, :, rows_of(p), :],
                got_c.at[p, x], c_sems, (p, i), device(c=other_c))

    def c_send(ps):
        for i in range(X):
            for p in ps:
                send(*c_link(p, i))

    def c_add(p):
        nf, mf, ng, mg = outer(p)
        for i in range(X):
            link(*c_link(p, i)).wait_recv()
        kind = pieces[p][0]
        for i in range(nf):
            f = away(mf, i + 1, nf)
            for j in range(ng):
                g = away(mg, j + 1, ng)
                x, y = xy(p, f, g)
                sum_f[p, i * ng + j] = part[kind, x, mc, :, y, rows_of(p), :] + got_c[p, x, :, y]

    def f_link(p, i, j):
        nf, mf, ng, mg = outer(p)
        slot = i * ng + j
        return (sum_f.at[p, slot], got_f.at[p, slot], f_sems, (p, slot),
                f_peer(p, away(mf, i + 1, nf)))

    def f_send(p):
        nf, mf, ng, mg = outer(p)
        for j in range(ng):
            for i in range(nf - 1):
                send(*f_link(p, i, j))

    def g_link(p, j):
        nf, mf, ng, mg = outer(p)
        return (sum_g.at[p, j], got_g.at[p, j], g_sems, (p, j),
                g_peer(p, away(mg, j + 1, ng)))

    def f_add(p, js):
        nf, mf, ng, mg = outer(p)
        for j in js:
            total = sum_f[p, (nf - 1) * ng + j]
            for i in range(nf - 1):
                link(*f_link(p, i, j)).wait_recv()
                total = total + got_f[p, i * ng + j]
            sum_g[p, j] = total
            if j < ng - 1:
                send(*g_link(p, j))

    def z_link(p, k):
        z = away(mz, k + 1, Z)
        return (sum_z.at[p, z], got_z.at[p, k], z_sems, (p, k), device(z=z))

    def g_add(p):
        nf, mf, ng, mg = outer(p)
        total = sum_g[p, ng - 1]
        for j in range(ng - 1):
            link(*g_link(p, j)).wait_recv()
            total = total + got_g[p, j]
        sum_z[p] = total
        for k in range(Z - 1):
            send(*z_link(p, k))

    def z_add(p):
        total = sum_z[p, mz]
        for k in range(Z - 1):
            link(*z_link(p, k)).wait_recv()
            total = total + got_z[p, k]
        return total

    def tile(p, x, c, z, y):
        return gathered.at[pieces[p][0], x, c, z, y, rows_of(p), :]

    def column(p, x, c, y):
        return gathered.at[pieces[p][0], x, c, :, y, rows_of(p), :]

    def zz_link(p, k, recv=False):
        z = away(mz, Z - 1 - k, Z) if recv else mz
        ref = tile(p, mx, mc, z, my)
        return (ref, ref, zz_sems, (p, k), device(z=away(mz, k + 1, Z)))

    def gg_link(p, j, k, recv=False):
        nf, mf, ng, mg = outer(p)
        g = away(mg, ng - 1 - j, ng) if recv else mg
        x, y = xy(p, mf, g)
        ref = tile(p, x, mc, away(mz, Z - k, Z), y)
        return (ref, ref, gg_sems, (p, j * Z + k), g_peer(p, away(mg, j + 1, ng)))

    def ff_link(p, i, j, recv=False):
        nf, mf, ng, mg = outer(p)
        f = away(mf, nf - 1 - i, nf) if recv else mf
        x, y = xy(p, f, away(mg, ng - j, ng))
        ref = column(p, x, mc, y)
        return (ref, ref, ff_sems, (p, i * ng + j), f_peer(p, away(mf, i + 1, nf)))

    def cc_link(p, i, j, recv=False):
        nf, mf, ng, mg = outer(p)
        x, y = xy(p, away(mf, nf - i, nf), away(mg, ng - j, ng))
        ref = column(p, x, other_c if recv else mc, y)
        return (ref, ref, cc_sems, (p, i * ng + j), device(c=other_c))

    def zz_send(p):
        nf, mf, ng, mg = outer(p)
        for k in range(Z - 1):
            send(*zz_link(p, k))
        for j in range(ng - 1):
            send(*gg_link(p, j, 0))

    def gg_send(p):
        nf, mf, ng, mg = outer(p)
        for k in range(Z - 1):
            link(*zz_link(p, k, True)).wait_recv()
            for j in range(ng - 1):
                send(*gg_link(p, j, k + 1))
        for i in range(nf - 1):
            send(*ff_link(p, i, 0))
        send(*cc_link(p, 0, 0))

    def ff_send(p):
        nf, mf, ng, mg = outer(p)
        for j in range(1, ng):
            for k in range(Z):
                link(*gg_link(p, j - 1, k, True)).wait_recv()
            for i in range(nf - 1):
                send(*ff_link(p, i, j))
            send(*cc_link(p, 0, j))

    def cc_send(p):
        nf, mf, ng, mg = outer(p)
        for j in range(ng):
            for i in range(1, nf):
                link(*ff_link(p, i - 1, j, True)).wait_recv()
                send(*cc_link(p, i, j))

    def cc_wait(p):
        nf, mf, ng, mg = outer(p)
        for i in range(nf):
            for j in range(ng):
                link(*cc_link(p, i, j, True)).wait_recv()

    def publish(p, value):
        gathered[pieces[p][0], mx, mc, mz, my, rows_of(p), :] = value
        zz_send(p)

    def own_curv(p):
        at = rows_of(p)
        prec = 0.5 * prec_old[at, :] + 0.5 * z_add(p)
        prec_out[at, :] = prec
        div = prec + 0.1 + 0.05
        divisor[at, :] = div
        publish(p, jnp.sqrt(0.3 / div))

    def own_grad(p):
        at = rows_of(p)
        mean = mean_old[at, :]
        mom = 0.9 * mom_old[at, :] + z_add(p) + 0.1 * mean
        mom_out[at, :] = mom
        new = mean - 0.3 * mom / divisor[at, :]
        mean_out[at, :] = new
        publish(p, new)

    curv = list(range(splits))
    grad = list(range(splits, 2 * splits))

    products(0, squared)
    pl.semaphore_wait(barrier, len(peers))
    c_send(curv)
    products(1, lambda values: values)
    c_send(grad)
    for p in curv:
        c_add(p)
        f_send(p)
    for p in grad:
        c_add(p)

    def halves(p):
        ng = outer(p)[2]
        return range(ng - 1), range(ng - 1, ng)

    for p in curv:
        f_add(p, halves(p)[0])
    for p in grad:
        f_send(p)
    for p in curv:
        f_add(p, halves(p)[1])
    for p in curv:
        g_add(p)
    for p in grad:
        f_add(p, halves(p)[0])
    for p in grad:
        f_add(p, halves(p)[1])
    for p in curv:
        own_curv(p)
    for p in grad:
        g_add(p)
    for p in curv:
        gg_send(p)
    for p in grad:
        own_grad(p)
    for p in curv:
        ff_send(p)
    for p in grad:
        gg_send(p)
    for p in curv:
        cc_send(p)
    for p in grad:
        ff_send(p)
    for p in grad:
        cc_send(p)
    for p in curv + grad:
        cc_wait(p)
    for copy in started:
        copy.wait_send()


def on_device(sizes, in_first, cot_first, in_third, cot_third, mean_old, prec_old, mom_old, noise):
    X, C, Z, Y, S, splits = sizes
    n, s = 2 * splits, S // splits
    shard = jax.ShapeDtypeStruct((S, LANES), jnp.float32)
    vmem = pl.BlockSpec(memory_space=pltpu.VMEM)
    wide = max(X, Y)

    def f32(*shape):
        return pltpu.VMEM(shape + (LANES,), jnp.float32)

    def sems(*shape):
        return pltpu.SemaphoreType.DMA((2, n) + shape)

    mean_new, prec_new, mom_new, both = pl.pallas_call(
        functools.partial(step_kernel, sizes),
        out_shape=(shard, shard, shard, jax.ShapeDtypeStruct((2, X, C, Z, Y, S, LANES), jnp.float32)),
        in_specs=[vmem] * 7,
        out_specs=[vmem] * 4,
        scratch_shapes=[
            f32(2, X, C, Z, Y, S),
            f32(n, X, Z, Y, s),
            f32(n, X * Y, Z, s),
            f32(n, X * Y, Z, s),
            f32(n, wide, Z, s),
            f32(n, wide, Z, s),
            f32(n, Z, s),
            f32(n, Z, s),
            f32(S),
            sems(X), sems(X * Y), sems(wide), sems(Z),
            sems(Z), sems(wide * Z), sems(X * Y), sems(X * Y),
        ],
        compiler_params=pltpu.CompilerParams(
            collective_id=0, has_side_effects=True, vmem_limit_bytes=48 * 1024 * 1024
        ),
    )(in_first, cot_first, in_third, cot_third,
      *(old.reshape(S, LANES) for old in (mean_old, prec_old, mom_old)))
    spread, mean = both[0].reshape(-1), both[1].reshape(-1)
    sample_row = (mean + spread * noise[0].astype(jnp.float32)).astype(jnp.bfloat16)
    return (mean_new.reshape(-1), prec_new.reshape(-1), mom_new.reshape(-1), sample_row.reshape(1, -1))


def solution(mesh):
    GX, GY, GZ = (mesh.shape[name] for name in AXES)
    split = P(AXES)
    rows = P(AXES, None)

    def whole_step(*arrays):
        params = arrays[4].shape[0]
        S = params // (GX * GY * GZ) // LANES
        sizes = (GX // 2, 2, GY, GZ, S, 2 if S % 16 == 0 else 1)
        return jax.shard_map(
            functools.partial(on_device, sizes),
            mesh=mesh,
            in_specs=(rows, rows, rows, rows, split, split, split, rows),
            out_specs=(split, split, split, rows),
            check_vma=False,
        )(*arrays)

    return whole_step
```

```python
import functools

import jax
import jax.numpy as jnp
from jax import lax
from jax.experimental import pallas as pl
from jax.experimental.pallas import tpu as pltpu
from jax.sharding import PartitionSpec as P

LANES = 128
BLOCK = 256
AXES = ("gx", "gy", "gz")


def squared(values):
    wide = values.astype(jnp.float32)
    return (wide * wide).astype(jnp.bfloat16)


def contract_rows(left, right):
    return lax.dot_general(
        left, right, (((0,), (0,)), ((), ())), preferred_element_type=jnp.float32
    )


def step_kernel(
    sizes,
    *refs,
):
    ins, refs = refs[:8], refs[8:]
    mean_out, prec_out, mom_out, samples = refs[:4]
    staged, refs = refs[4:12], refs[12:]
    in_first, cot_first, in_third, cot_third, mean_old, prec_old, mom_old, noise = staged
    (
    gathered, part, got_c, sum_f, got_f, sum_g, got_g, sum_z, got_z, divisor,
    c_sems, f_sems, g_sems, z_sems, zz_sems, gg_sems, ff_sems, cc_sems, in_sems,
    ) = refs
    loads = [pltpu.make_async_copy(ins[i], staged[i], in_sems.at[i]) for i in range(8)]
    for load in loads:
        load.start()

    X, C, Z, Y, S, splits = sizes
    s = S // splits
    gx, mz, my = (lax.axis_index(name) for name in AXES)
    mx, mc = gx // C, lax.rem(gx, C)
    other_c = 1 - mc

    def device(x=None, c=None, z=None, y=None):
        x = mx if x is None else x
        c = mc if c is None else c
        return (x * C + c, mz if z is None else z, my if y is None else y)

    def away(mine, step, size):
        return lax.rem(mine + step, size)

    barrier = pltpu.get_barrier_semaphore()
    peers = [device(c=other_c)]
    peers += [device(x=away(mx, k, X)) for k in range(1, X)]
    peers += [device(y=away(my, k, Y)) for k in range(1, Y)]
    peers += [device(z=away(mz, k, Z)) for k in range(1, Z)]
    for peer in peers:
        pl.semaphore_signal(barrier, inc=1, device_id=peer, device_id_type=pl.DeviceIdType.MESH)

    started = []

    def link(src, dst, sems, index, peer):
        return pltpu.make_async_remote_copy(
            src_ref=src, dst_ref=dst,
            send_sem=sems.at[(0,) + index], recv_sem=sems.at[(1,) + index],
            device_id=peer, device_id_type=pl.DeviceIdType.MESH,
        )

    def send(*args):
        copy = link(*args)
        copy.start()
        started.append(copy)

    def place(index):
        rest, y = divmod(index, Y)
        rest, z = divmod(rest, Z)
        x, c = divmod(rest, C)
        return x, c, z, y

    def put(kind, base, block, row0, col0, width):
        rows = S * LANES // width
        across = width // LANES
        for i in range(block.shape[0] // rows):
            x, c, z, y = place(base + row0 // rows + i)
            for j in range(block.shape[1] // LANES):
                part[kind, x, c, z, y, pl.ds(col0 // LANES + j, rows, stride=across), :] = (
                    block[i * rows:(i + 1) * rows, j * LANES:(j + 1) * LANES]
                )

    def products(kind, shape):
        cin, mid = in_first.shape[1], cot_first.shape[1]
        if kind == 0:
            loads[0].wait()
            loads[1].wait()
        right = shape(cot_first[...])
        for r in range(0, cin, BLOCK):
            put(kind, 0, contract_rows(shape(in_first[:, r:r + BLOCK]), right), r, 0, mid)
        base = X * C * Z * Y // 2
        if kind == 0:
            loads[2].wait()
            loads[3].wait()
        left = shape(in_third[...])
        for r in range(0, cin, BLOCK):
            put(kind, base, contract_rows(left, shape(cot_third[:, r:r + BLOCK])), 0, r, cin)

    pieces = [(kind, split) for kind in (0, 1) for split in range(splits)]
    flip = [(kind + split) % 2 if splits == 1 else split % 2 for kind, split in pieces]

    def rows_of(p):
        split = pieces[p][1]
        return pl.ds(split * s, s)

    def outer(p):
        return (Y, my, X, mx) if flip[p] else (X, mx, Y, my)

    def xy(p, f, g):
        return (g, f) if flip[p] else (f, g)

    def f_peer(p, f):
        return device(y=f) if flip[p] else device(x=f)

    def g_peer(p, g):
        return device(x=g) if flip[p] else device(y=g)

    def c_link(p, i):
        x = away(mx, i + 1, X)
        return (part.at[pieces[p][0], x, other_c, :, :, rows_of(p), :],
                got_c.at[p, x], c_sems, (p, i), device(c=other_c))

    def c_send(ps):
        for i in range(X):
            for p in ps:
                send(*c_link(p, i))

    def c_add(p):
        nf, mf, ng, mg = outer(p)
        for i in range(X):
            link(*c_link(p, i)).wait_recv()
        kind = pieces[p][0]
        for i in range(nf):
            f = away(mf, i + 1, nf)
            for j in range(ng):
                g = away(mg, j + 1, ng)
                x, y = xy(p, f, g)
                sum_f[p, i * ng + j] = part[kind, x, mc, :, y, rows_of(p), :] + got_c[p, x, :, y]

    def f_link(p, i, j):
        nf, mf, ng, mg = outer(p)
        slot = i * ng + j
        return (sum_f.at[p, slot], got_f.at[p, slot], f_sems, (p, slot),
                f_peer(p, away(mf, i + 1, nf)))

    def f_send(p):
        nf, mf, ng, mg = outer(p)
        for j in range(ng):
            for i in range(nf - 1):
                send(*f_link(p, i, j))

    def g_link(p, j):
        nf, mf, ng, mg = outer(p)
        return (sum_g.at[p, j], got_g.at[p, j], g_sems, (p, j),
                g_peer(p, away(mg, j + 1, ng)))

    def f_add(p, js):
        nf, mf, ng, mg = outer(p)
        for j in js:
            total = sum_f[p, (nf - 1) * ng + j]
            for i in range(nf - 1):
                link(*f_link(p, i, j)).wait_recv()
                total = total + got_f[p, i * ng + j]
            sum_g[p, j] = total
            if j < ng - 1:
                send(*g_link(p, j))

    def z_link(p, k):
        z = away(mz, k + 1, Z)
        return (sum_z.at[p, z], got_z.at[p, k], z_sems, (p, k), device(z=z))

    def g_add(p):
        nf, mf, ng, mg = outer(p)
        total = sum_g[p, ng - 1]
        for j in range(ng - 1):
            link(*g_link(p, j)).wait_recv()
            total = total + got_g[p, j]
        sum_z[p] = total
        for k in range(Z - 1):
            send(*z_link(p, k))

    def z_add(p):
        total = sum_z[p, mz]
        for k in range(Z - 1):
            link(*z_link(p, k)).wait_recv()
            total = total + got_z[p, k]
        return total

    def tile(p, x, c, z, y):
        return gathered.at[pieces[p][0], x, c, z, y, rows_of(p), :]

    def column(p, x, c, y):
        return gathered.at[pieces[p][0], x, c, :, y, rows_of(p), :]

    def zz_link(p, k, recv=False):
        z = away(mz, Z - 1 - k, Z) if recv else mz
        ref = tile(p, mx, mc, z, my)
        return (ref, ref, zz_sems, (p, k), device(z=away(mz, k + 1, Z)))

    def gg_link(p, j, k, recv=False):
        nf, mf, ng, mg = outer(p)
        g = away(mg, ng - 1 - j, ng) if recv else mg
        x, y = xy(p, mf, g)
        ref = tile(p, x, mc, away(mz, Z - k, Z), y)
        return (ref, ref, gg_sems, (p, j * Z + k), g_peer(p, away(mg, j + 1, ng)))

    def ff_link(p, i, j, recv=False):
        nf, mf, ng, mg = outer(p)
        f = away(mf, nf - 1 - i, nf) if recv else mf
        x, y = xy(p, f, away(mg, ng - j, ng))
        ref = column(p, x, mc, y)
        return (ref, ref, ff_sems, (p, i * ng + j), f_peer(p, away(mf, i + 1, nf)))

    def cc_link(p, i, j, recv=False):
        nf, mf, ng, mg = outer(p)
        x, y = xy(p, away(mf, nf - i, nf), away(mg, ng - j, ng))
        ref = column(p, x, other_c if recv else mc, y)
        return (ref, ref, cc_sems, (p, i * ng + j), device(c=other_c))

    def zz_send(p):
        nf, mf, ng, mg = outer(p)
        for k in range(Z - 1):
            send(*zz_link(p, k))
        for j in range(ng - 1):
            send(*gg_link(p, j, 0))

    def gg_send(p):
        nf, mf, ng, mg = outer(p)
        for k in range(Z - 1):
            link(*zz_link(p, k, True)).wait_recv()
            for j in range(ng - 1):
                send(*gg_link(p, j, k + 1))
        for i in range(nf - 1):
            send(*ff_link(p, i, 0))
        send(*cc_link(p, 0, 0))

    def ff_send(p):
        nf, mf, ng, mg = outer(p)
        for j in range(1, ng):
            for k in range(Z):
                link(*gg_link(p, j - 1, k, True)).wait_recv()
            for i in range(nf - 1):
                send(*ff_link(p, i, j))
            send(*cc_link(p, 0, j))

    def cc_send(p):
        nf, mf, ng, mg = outer(p)
        for j in range(ng):
            for i in range(1, nf):
                link(*ff_link(p, i - 1, j, True)).wait_recv()
                send(*cc_link(p, i, j))

    def cc_wait(p, i):
        for j in range(outer(p)[2]):
            link(*cc_link(p, i, j, True)).wait_recv()

    def sample(p, i, j, c):
        nf, mf, ng, mg = outer(p)
        split = pieces[p][1]
        x, y = xy(p, away(mf, nf - i, nf), away(mg, ng - j, ng))
        for z in range(Z):
            row = (((x * C + c) * Z + z) * Y + y) * S + split * s
            at = pl.ds(pl.multiple_of(row * LANES, s * LANES), s * LANES)
            normal = noise[0, at].astype(jnp.float32).reshape(s, LANES)
            value = (gathered[1, x, c, z, y, rows_of(p), :]
                     + gathered[0, x, c, z, y, rows_of(p), :] * normal)
            samples[0, at] = value.astype(jnp.bfloat16).reshape(s * LANES)

    def publish(p, value):
        gathered[pieces[p][0], mx, mc, mz, my, rows_of(p), :] = value
        zz_send(p)

    def own_curv(p):
        at = rows_of(p)
        prec = 0.5 * prec_old[at, :] + 0.5 * z_add(p)
        prec_out[at, :] = prec
        div = prec + 0.1 + 0.05
        divisor[at, :] = div
        publish(p, jnp.sqrt(0.3 / div))

    def own_grad(p):
        at = rows_of(p)
        mean = mean_old[at, :]
        mom = 0.9 * mom_old[at, :] + z_add(p) + 0.1 * mean
        mom_out[at, :] = mom
        new = mean - 0.3 * mom / divisor[at, :]
        mean_out[at, :] = new
        publish(p, new)

    curv = list(range(splits))
    grad = list(range(splits, 2 * splits))

    products(0, squared)
    pl.semaphore_wait(barrier, len(peers))
    c_send(curv)
    products(1, lambda values: values)
    c_send(grad)
    for p in curv:
        c_add(p)
        f_send(p)
    for p in grad:
        c_add(p)

    def halves(p):
        ng = outer(p)[2]
        return range(ng - 1), range(ng - 1, ng)

    for p in curv:
        f_add(p, halves(p)[0])
    for p in grad:
        f_send(p)
    for p in curv:
        f_add(p, halves(p)[1])
    for p in curv:
        g_add(p)
    for p in grad:
        f_add(p, halves(p)[0])
    for p in grad:
        f_add(p, halves(p)[1])
    for load in loads[4:7]:
        load.wait()
    for p in curv:
        own_curv(p)
    for p in grad:
        g_add(p)
    for p in curv:
        gg_send(p)
    for p in grad:
        own_grad(p)
    for p in curv:
        ff_send(p)
    for p in grad:
        gg_send(p)
    for p in curv:
        cc_send(p)
    loads[7].wait()
    same = splits > 1
    for p in grad:
        if same:
            sample(p, 0, 0, mc)
    for p in grad:
        ff_send(p)
    for p in curv:
        for i in range(outer(p)[0]):
            cc_wait(p, i)
    if same:
        for p in grad:
            for j in range(1, outer(p)[2]):
                sample(p, 0, j, mc)
        for p in grad:
            cc_wait(p, 0)
            for j in range(outer(p)[2]):
                sample(p, 0, j, other_c)
    for p in grad:
        cc_send(p)
    if same:
        for p in grad:
            for i in range(1, outer(p)[0]):
                for j in range(outer(p)[2]):
                    sample(p, i, j, mc)
    for p in grad:
        for i in range(1 if same else 0, outer(p)[0]):
            cc_wait(p, i)
            if same:
                for j in range(outer(p)[2]):
                    sample(p, i, j, other_c)
    if not same:
        for p in grad:
            for i in range(outer(p)[0]):
                for j in range(outer(p)[2]):
                    for c in range(C):
                        sample(p, i, j, c)
    for copy in started:
        copy.wait_send()


def on_device(sizes, in_first, cot_first, in_third, cot_third, mean_old, prec_old, mom_old, noise):
    X, C, Z, Y, S, splits = sizes
    n, s = 2 * splits, S // splits
    shard = jax.ShapeDtypeStruct((S, LANES), jnp.float32)
    vmem = pl.BlockSpec(memory_space=pltpu.VMEM)
    wide = max(X, Y)

    def f32(*shape):
        return pltpu.VMEM(shape + (LANES,), jnp.float32)

    def sems(*shape):
        return pltpu.SemaphoreType.DMA((2, n) + shape)

    inputs = (in_first, cot_first, in_third, cot_third,
              *(old.reshape(S, LANES) for old in (mean_old, prec_old, mom_old)), noise)
    mean_new, prec_new, mom_new, sample_row = pl.pallas_call(
        functools.partial(step_kernel, sizes),
        out_shape=(shard, shard, shard, jax.ShapeDtypeStruct(noise.shape, jnp.bfloat16)),
        in_specs=[pl.BlockSpec(memory_space=pltpu.HBM)] * 8,
        out_specs=[vmem] * 4,
        scratch_shapes=[
            *(pltpu.VMEM(value.shape, value.dtype) for value in inputs),
            f32(2, X, C, Z, Y, S),
            f32(2, X, C, Z, Y, S),
            f32(n, X, Z, Y, s),
            f32(n, X * Y, Z, s),
            f32(n, X * Y, Z, s),
            f32(n, wide, Z, s),
            f32(n, wide, Z, s),
            f32(n, Z, s),
            f32(n, Z, s),
            f32(S),
            sems(X), sems(X * Y), sems(wide), sems(Z),
            sems(Z), sems(wide * Z), sems(X * Y), sems(X * Y),
            pltpu.SemaphoreType.DMA((8,)),
        ],
        compiler_params=pltpu.CompilerParams(
            collective_id=0, has_side_effects=True, vmem_limit_bytes=40 * 1024 * 1024
        ),
    )(*(pltpu.with_memory_space_constraint(value, pltpu.HBM) for value in inputs))
    return (mean_new.reshape(-1), prec_new.reshape(-1), mom_new.reshape(-1), sample_row)


def solution(mesh):
    GX, GY, GZ = (mesh.shape[name] for name in AXES)
    split = P(AXES)
    rows = P(AXES, None)

    def whole_step(*arrays):
        params = arrays[4].shape[0]
        S = params // (GX * GY * GZ) // LANES
        sizes = (GX // 2, 2, GY, GZ, S, 2 if S % 16 == 0 else 1)
        return jax.shard_map(
            functools.partial(on_device, sizes),
            mesh=mesh,
            in_specs=(rows, rows, rows, rows, split, split, split, rows),
            out_specs=(split, split, split, rows),
            check_vma=False,
        )(*arrays)

    return whole_step
```
